1024 devices in a mesh: gx: 16 (over y, z_hi), gy: 8 (over z_lo), gz: 8 (over x, core).
Axes of the slice: x: 4, y: 4, z: 32 (z_hi: 4, z_lo: 8; z = z_hi * 8 + z_lo), core: 2. Of those that a mesh axis runs over, the one named last changes fastest.
Arguments:
- populations: float32 [19, 128, 64, 1024], P(None, 'gx', 'gy', 'gz'), may hold values from 0.01 to 0.11
Outputs:
- populations_next: float32 [19, 128, 64, 1024], P(None, 'gx', 'gy', 'gz')
- moments_slab: float32 [4, 1024, 64, 128], P(None, ('gz', 'gx'), 'gy')
The draws below stay inside these ranges and needn't reach their ends.
All inputs are finite; a program needn't handle non-finite values.
Results may differ from the reference program's by a relative error of at most 0.0003.
Values sent between devices are 32-bit elements; how exact they have to be, the bound alone decides.
No kernel may reach another device: no remote copies, remote signals or barrier semaphores. Data moves between devices by JAX's collectives and lax.ppermute only.
A program may use at most 32 MiB of HBM per device.

```python
from functools import reduce
import jax
import jax.numpy as jnp

Q = 19
NX = 128
NY = 64
NZ = 1024


def levels(key, dims, cuts, least, largest):
    loudness = 1.0
    for position, parts in cuts:
        heights = jax.random.uniform(jax.random.fold_in(jax.random.fold_in(key, 6), position), (parts,), jnp.float32, least / len(cuts), largest / len(cuts))
        loudness = loudness * jnp.repeat(jnp.exp(heights), dims[position] // parts).reshape((-1,) + (1,) * (len(dims) - 1 - position))
    return loudness


def setup_inputs(seed: int = 0) -> dict:
    seeds = jax.random.split(jax.random.key(seed), 2)
    populations = jnp.clip(0.01 + 0.1 * jax.random.uniform(seeds[0], (Q, NX, NY, NZ), jnp.float32) ** levels(seeds[0], (Q, NX, NY, NZ), ((1, 16), (2, 8), (3, 8)), -0.2, 0.2), 0.01, 0.11)
    return dict(populations=populations)


lattice_moves = [(0, 0, 0), (1, 0, 0), (-1, 0, 0), (0, 1, 0), (0, -1, 0), (0, 0, 1), (0, 0, -1),
                 (1, 1, 0), (-1, -1, 0), (1, -1, 0), (-1, 1, 0), (1, 0, 1), (-1, 0, -1), (1, 0, -1), (-1, 0, 1),
                 (0, 1, 1), (0, -1, -1), (0, 1, -1), (0, -1, 1)]
lattice_weights = [1.0 / 3.0] + [1.0 / 18.0] * 6 + [1.0 / 36.0] * 12
relaxation = 1.6


def signed_total(pieces, component):
    total = jnp.zeros_like(pieces[0])
    for move, piece in zip(lattice_moves, pieces):
        if move[component] == 1:
            total = total + piece
        elif move[component] == -1:
            total = total - piece
    return total


def lattice_moments(pieces):
    density = reduce(lambda left, right: left + right, pieces)
    velocity_x = signed_total(pieces, 0) / density
    velocity_y = signed_total(pieces, 1) / density
    velocity_z = signed_total(pieces, 2) / density
    return density, velocity_x, velocity_y, velocity_z


def collide(pieces):
    density, velocity_x, velocity_y, velocity_z = lattice_moments(pieces)
    speed_sq = velocity_x * velocity_x + velocity_y * velocity_y + velocity_z * velocity_z
    result = []
    for move, weight, piece in zip(lattice_moves, lattice_weights, pieces):
        projected = move[0] * velocity_x + move[1] * velocity_y + move[2] * velocity_z
        balance = weight * density * (1.0 + 3.0 * projected + 4.5 * projected * projected - 1.5 * speed_sq)
        result.append(piece - relaxation * (piece - balance))
    return result


def reference(populations):
    pieces = [populations[index] for index in range(19)]
    moments = jnp.stack(lattice_moments(pieces))
    moments_slab = jnp.transpose(moments, (0, 3, 2, 1))
    read = [jnp.roll(pieces[index], lattice_moves[index], axis=(0, 1, 2)) for index in range(19)]
    populations_next = jnp.stack(collide(read))
    return populations_next, moments_slab
```

```python
import jax
import jax.numpy as jnp
from jax import lax
from jax.experimental import pallas as pl
from jax.experimental.pallas import tpu as pltpu
from jax.sharding import PartitionSpec as P

lattice_moves = [
    (0, 0, 0),
    (1, 0, 0),
    (-1, 0, 0),
    (0, 1, 0),
    (0, -1, 0),
    (0, 0, 1),
    (0, 0, -1),
    (1, 1, 0),
    (-1, -1, 0),
    (1, -1, 0),
    (-1, 1, 0),
    (1, 0, 1),
    (-1, 0, -1),
    (1, 0, -1),
    (-1, 0, 1),
    (0, 1, 1),
    (0, -1, -1),
    (0, 1, -1),
    (0, -1, 1),
]
lattice_weights = [1.0 / 3.0] + [1.0 / 18.0] * 6 + [1.0 / 36.0] * 12
relaxation = 1.6
TILE = (8, 128)
f32 = jnp.float32


def moving(axis, sign):
    return [i for i, move in enumerate(lattice_moves) if move[axis] == sign]


XP, XM = moving(0, 1), moving(0, -1)
YP, YM = moving(1, 1), moving(1, -1)
ZP, ZM = moving(2, 1), moving(2, -1)


def lanes():
    return lax.broadcasted_iota(jnp.int32, TILE, 1)


def rows():
    return lax.broadcasted_iota(jnp.int32, TILE, 0)


def roll_lanes(tile, shift):
    shift %= 128
    return pltpu.roll(tile, shift, axis=1) if shift else tile


def roll_rows(tile, shift):
    shift %= 8
    return pltpu.roll(tile, shift, axis=0) if shift else tile


def momenta(pieces):
    density = pieces[0]
    for piece in pieces[1:]:
        density = density + piece
    sums = []
    for axis in range(3):
        ups, downs = [pieces[i] for i in moving(axis, 1)], [pieces[i] for i in moving(axis, -1)]
        total = ups[0] - downs[0]
        for up, down in zip(ups[1:], downs[1:]):
            total = total + (up - down)
        sums.append(total)
    inverse = 1.0 / density
    return [density] + [total * inverse for total in sums]


def swap_lane_groups(tiles, width):
    tiles, step, lane = list(tiles), 1, lanes()
    while step < len(tiles):
        low = (lane // (width * step)) % 2 == 0
        for a in range(len(tiles)):
            if not a & step:
                b = a + step
                one, two = tiles[a], tiles[b]
                tiles[a] = jnp.where(low, one, roll_lanes(two, width * step))
                tiles[b] = jnp.where(low, roll_lanes(one, -width * step), two)
        step *= 2
    return tiles


def pre_kernel(zhi_ref, pops_ref, own_ref, up_ref, far_ref, down_ref, zp_ref, zm_ref, parcels):
    lane = lanes()
    for faces, out, edge in ((ZP, zp_ref, 127), (ZM, zm_ref, 0)):
        tile = jnp.zeros(TILE, f32)
        for q, i in enumerate(faces):
            for x in range(8):
                column = q * 8 + x
                tile = jnp.where(lane == column, roll_lanes(pops_ref[i, x], column - edge), tile)
        out[...] = tile
    fields = [momenta([pops_ref[i, x] for i in range(19)]) for x in range(8)]
    planes = [swap_lane_groups([fields[x][m] for x in range(8)], 1) for m in range(4)]
    for half in range(2):
        sixteen = swap_lane_groups(planes[2 * half] + planes[2 * half + 1], 8)
        for part in range(16):
            parcels[part % 4, part // 4 * 2 + half] = sixteen[part]
    zhi = zhi_ref[0]
    for shift, out in enumerate((own_ref, up_ref, far_ref, down_ref)):
        target = lax.rem(zhi + shift, 4)
        for k in range(8):
            out[k] = parcels[target, k]
    for faces, out, x in ((XP, up_ref, 7), (XM, down_ref, 0)):
        for q, i in enumerate(faces):
            out[8 + q] = pops_ref[i, x]
        out[13] = jnp.zeros(TILE, f32)


def edge_kernel(zp_ref, zm_ref, up_in, down_in, up_ref, down_ref):
    edge = jnp.where(lanes() < 64, zp_ref[...], roll_lanes(zm_ref[...], 64))
    for source, out in ((up_in, up_ref), (down_in, down_ref)):
        out[0:13] = source[0:13]
        out[13] = edge


def mid_kernel(pops_ref, own_ref, up_ref, far_ref, down_ref, zp_ref, zm_ref, load_ref, yp_ref, ym_ref):
    row = rows()
    for y in range(4):
        for r, source in enumerate((own_ref, up_ref, far_ref, down_ref)):
            for half in range(2):
                load_ref[y, r * 2 + half] = source[y * 2 + half]
    ways = (
        (YP, yp_ref, 7, (up_ref[8 + XP.index(7)], down_ref[8 + XM.index(10)], zp_ref[...], zm_ref[...])),
        (YM, ym_ref, 0, (down_ref[8 + XM.index(8)], up_ref[8 + XP.index(9)], zm_ref[...], zp_ref[...])),
    )
    for faces, out, y, extra in ways:
        for q, i in enumerate(faces):
            tile = jnp.zeros(TILE, f32)
            for x in range(8):
                tile = jnp.where(row == x, roll_rows(pops_ref[i, x], x - y), tile)
            out[q] = tile
        tile = jnp.zeros(TILE, f32)
        for k, source in enumerate(extra):
            tile = jnp.where(row == k, roll_rows(source, k - y), tile)
        out[5] = tile


def spread(tile, k):
    return jnp.broadcast_to(tile[k : k + 1, :], TILE)


def collide_kernel(pops_ref, zp_ref, zm_ref, up_ref, down_ref, yp_ref, ym_ref, out_ref):
    lane, row = lanes(), rows()
    zcol = {1: (ZP, zp_ref[...]), -1: (ZM, zm_ref[...])}
    xface = {1: (XP, up_ref), -1: (XM, down_ref)}
    yface = {1: (YP, yp_ref), -1: (YM, ym_ref)}
    first_row = {1: row == 7, -1: row == 0}
    first_lane = {1: lane == 127, -1: lane == 0}
    edge_rows = {7: (1, 0), 10: (1, 1), 8: (-1, 0), 9: (-1, 1), 15: (1, 2), 17: (1, 3), 16: (-1, 2), 18: (-1, 3)}
    corner = {}
    for i in (15, 16, 17, 18):
        way, k = edge_rows[i]
        cy, cz = lattice_moves[i][1], lattice_moves[i][2]
        corner[i] = jnp.where(first_row[cy], spread(yface[way][1][5], k), zcol[cz][1])
    for x in range(8):
        read = []
        for i, (cx, cy, cz) in enumerate(lattice_moves):
            source = x - cx
            inside = 0 <= source < 8
            if inside:
                tile = pops_ref[i, source]
            else:
                faces, ref = xface[cx]
                tile = ref[8 + faces.index(i)]
            if cy:
                faces, ref = yface[cy]
                if inside:
                    line = spread(ref[faces.index(i)], source)
                else:
                    line = spread(ref[5], edge_rows[i][1])
                tile = jnp.where(first_row[cy], line, tile)
            if cz:
                faces, column = zcol[cz]
                if cy:
                    column = corner[i]
                at = faces.index(i) * 8 + source % 8
                if not inside:
                    at += 0 if cz == 1 else 64
                    column = xface[cx][1][13]
                tile = jnp.where(first_lane[cz], roll_lanes(column, (127 if cz == 1 else 0) - at), tile)
                tile = roll_lanes(tile, cz)
            if cy:
                tile = roll_rows(tile, cy)
            read.append(tile)
        density, ux, uy, uz = momenta(read)
        common = 1.0 - 1.5 * (ux * ux + uy * uy + uz * uz)
        scaled = {w: (relaxation * w) * density for w in sorted(set(lattice_weights))}
        keep = 1.0 - relaxation
        out_ref[0, x] = keep * read[0] + scaled[lattice_weights[0]] * common
        for i in range(1, 19, 2):
            projected = None
            for c, u in zip(lattice_moves[i], (ux, uy, uz)):
                if c:
                    term = u if c == 1 else -u
                    projected = term if projected is None else projected + term
            weight = scaled[lattice_weights[i]]
            even = weight * (common + 4.5 * projected * projected)
            odd = weight * (3.0 * projected)
            out_ref[i, x] = keep * read[i] + (even + odd)
            out_ref[i + 1, x] = keep * read[i + 1] + (even - odd)


def post_kernel(zhi_ref, load_ref, out_ref):
    turn = zhi_ref[0] * 8
    for half in range(2):
        tiles = [None] * 16
        for y in range(4):
            for r, shift in enumerate((0, 1, 2, -1)):
                tiles[(4 * y - shift) % 16] = load_ref[y, r * 2 + half]
        for k, tile in enumerate(swap_lane_groups(tiles, 8)):
            out_ref[2 * half + k // 8, k % 8] = pltpu.roll(tile, turn, axis=1)


def call(kernel, out_shapes, n_scalars, args, scratch=()):
    vmem = pl.BlockSpec(memory_space=pltpu.VMEM)
    smem = pl.BlockSpec(memory_space=pltpu.SMEM)
    return pl.pallas_call(
        kernel,
        out_shape=[jax.ShapeDtypeStruct(s, f32) for s in out_shapes],
        in_specs=[smem] * n_scalars + [vmem] * (len(args) - n_scalars),
        out_specs=[vmem] * len(out_shapes),
        scratch_shapes=list(scratch),
        compiler_params=pltpu.CompilerParams(vmem_limit_bytes=16 * 1024 * 1024),
        name=kernel.__name__,
    )(*args)


def shifted(x, axis, by):
    count = lax.axis_size(axis)
    return lax.ppermute(x, axis, [(i, (i + by) % count) for i in range(count)])


def on_device(populations):
    zhi = lax.rem(lax.axis_index("gx"), 4).reshape(1)
    own, up, far, down, zp, zm = call(
        pre_kernel,
        [(8, 8, 128), (14, 8, 128), (8, 8, 128), (14, 8, 128), TILE, TILE],
        1,
        (zhi, populations),
        [pltpu.VMEM((4, 8, 8, 128), f32)],
    )
    zp, zm = shifted(zp, "gz", 1), shifted(zm, "gz", -1)
    far = shifted(far, "gx", 2)
    up, down = call(edge_kernel, [(14, 8, 128)] * 2, 0, (zp, zm, up, down))
    up, down = shifted(up, "gx", 1), shifted(down, "gx", -1)
    load, yp, ym = call(
        mid_kernel,
        [(4, 8, 8, 128), (6, 8, 128), (6, 8, 128)],
        0,
        (populations, own, up, far, down, zp, zm),
    )
    yp, ym = shifted(yp, "gy", 1), shifted(ym, "gy", -1)
    groups = [[y * 4 + z for y in range(4)] for z in range(4)]
    load = lax.all_to_all(
        load.reshape(4, 8192), "gx", 0, 0, tiled=True, axis_index_groups=groups
    ).reshape(4, 8, 8, 128)
    (populations_next,) = call(
        collide_kernel, [(19, 8, 8, 128)], 0, (populations, zp, zm, up, down, yp, ym)
    )
    (moments_slab,) = call(post_kernel, [(4, 8, 8, 128)], 1, (zhi, load))
    return (populations_next, moments_slab)


def solution(mesh):
    return jax.shard_map(
        on_device,
        mesh=mesh,
        in_specs=(P(None, "gx", "gy", "gz"),),
        out_specs=(P(None, "gx", "gy", "gz"), P(None, ("gz", "gx"), "gy", None)),
        check_vma=False,
    )
```

```python
from functools import reduce

import jax
import jax.numpy as jnp
from jax import lax
from jax.experimental import pallas as pl
from jax.experimental.pallas import tpu as pltpu
from jax.sharding import PartitionSpec as P


lattice_moves = [
    (0, 0, 0),
    (1, 0, 0),
    (-1, 0, 0),
    (0, 1, 0),
    (0, -1, 0),
    (0, 0, 1),
    (0, 0, -1),
    (1, 1, 0),
    (-1, -1, 0),
    (1, -1, 0),
    (-1, 1, 0),
    (1, 0, 1),
    (-1, 0, -1),
    (1, 0, -1),
    (-1, 0, 1),
    (0, 1, 1),
    (0, -1, -1),
    (0, 1, -1),
    (0, -1, 1),
]
lattice_weights = [1.0 / 3.0] + [1.0 / 18.0] * 6 + [1.0 / 36.0] * 12
relaxation = 1.6
TILE = (8, 128)
SHIFTS = (0, 1, 2, -1)
LONG = (
    ("far", {2: 2, 3: 2, 0: -1, 1: 1}),
    ("up", {0: 1, 1: 1, 2: 1, 3: 1}),
    ("down", {0: -1, 1: -1, 2: -1, 3: -1}),
    ("relay", {2: 1, 3: -1}),
)
PASSING = {"far": (2, 3)}
f32 = jnp.float32


def moving(axis, sign):
    return [i for i, move in enumerate(lattice_moves) if move[axis] == sign]


XP, XM = moving(0, 1), moving(0, -1)
YP, YM = moving(1, 1), moving(1, -1)
ZP, ZM = moving(2, 1), moving(2, -1)


def lanes():
    return lax.broadcasted_iota(jnp.int32, TILE, 1)


def rows():
    return lax.broadcasted_iota(jnp.int32, TILE, 0)


def roll_lanes(tile, shift):
    shift %= 128
    return pltpu.roll(tile, shift, axis=1) if shift else tile


def roll_rows(tile, shift):
    shift %= 8
    return pltpu.roll(tile, shift, axis=0) if shift else tile


def momenta(pieces):
    density = pieces[0]
    for piece in pieces[1:]:
        density = density + piece
    sums = []
    for axis in range(3):
        ups, downs = [pieces[i] for i in moving(axis, 1)], [pieces[i] for i in moving(axis, -1)]
        total = ups[0] - downs[0]
        for up, down in zip(ups[1:], downs[1:]):
            total = total + (up - down)
        sums.append(total)
    inverse = 1.0 / density
    return [density] + [total * inverse for total in sums]


def swap_lane_groups(tiles, width):
    tiles, step, lane = list(tiles), 1, lanes()
    while step < len(tiles):
        low = (lane // (width * step)) % 2 == 0
        for a in range(len(tiles)):
            if not a & step:
                b = a + step
                one, two = tiles[a], tiles[b]
                tiles[a] = jnp.where(low, one, roll_lanes(two, width * step))
                tiles[b] = jnp.where(low, roll_lanes(one, -width * step), two)
        step *= 2
    return tiles


def face_columns(pops_ref, faces, edge):
    tile = jnp.zeros(TILE, f32)
    for q, i in enumerate(faces):
        for x in range(8):
            column = q * 8 + x
            tile = jnp.where(lanes() == column, roll_lanes(pops_ref[i, x], column - edge), tile)
    return tile


def z_kernel(pops_ref, zp_ref, zm_ref):
    zp_ref[...] = face_columns(pops_ref, ZP, 127)
    zm_ref[...] = face_columns(pops_ref, ZM, 0)


def pre_kernel(pops_ref, load_ref, parcels):
    fields = [momenta([pops_ref[i, x] for i in range(19)]) for x in range(8)]
    planes = [swap_lane_groups([fields[x][m] for x in range(8)], 1) for m in range(4)]
    for half in range(2):
        sixteen = swap_lane_groups(planes[2 * half] + planes[2 * half + 1], 8)
        for part in range(16):
            parcels[part, half] = sixteen[part]
    zhi = lax.rem(lax.axis_index("gx"), 4)
    for y in range(4):
        for r, shift in enumerate(SHIFTS):
            if shift == 2:
                shift = jnp.where(zhi == 0, -2, 2)
            part = lax.rem(zhi + (4 * y + shift + 16), 16)
            for half in range(2):
                load_ref[y, r * 2 + half] = parcels[part, half]


def along_z(tile, i, x, columns):
    cz = lattice_moves[i][2]
    if not cz:
        return tile
    faces, column = columns[cz]
    at, edge = faces.index(i) * 8 + x, 127 if cz == 1 else 0
    return roll_lanes(jnp.where(lanes() == edge, roll_lanes(column, edge - at), tile), cz)


def along_y(tile, i, x, lines):
    cy = lattice_moves[i][1]
    if not cy:
        return tile
    faces, tiles = lines[cy]
    line = jnp.broadcast_to(tiles[faces.index(i)][x : x + 1, :], TILE)
    return roll_rows(jnp.where(rows() == (7 if cy == 1 else 0), line, tile), cy)


def y_kernel(pops_ref, zp_ref, zm_ref, first_ref, second_ref, work_ref):
    columns = {1: (ZP, zp_ref[...]), -1: (ZM, zm_ref[...])}
    for faces, out, y in ((YP, work_ref.at[1], 7), (YM, work_ref.at[0], 0)):
        for q, i in enumerate(faces):
            tile = jnp.zeros(TILE, f32)
            for x in range(8):
                line = along_z(pops_ref[i, x], i, x, columns)
                tile = jnp.where(rows() == x, roll_rows(line, x - y), tile)
            out[q] = tile
    odd = lax.rem(lax.axis_index("gy"), 2)
    first_ref[...] = work_ref[odd]
    second_ref[...] = work_ref[1 - odd]


def y_lines(first_ref, second_ref):
    odd = lax.rem(lax.axis_index("gy"), 2) == 1
    lines = {}
    for sign, faces in ((1, YP), (-1, YM)):
        one, two = (first_ref, second_ref) if sign == 1 else (second_ref, first_ref)
        lines[sign] = (faces, [jnp.where(odd, two[q], one[q]) for q in range(5)])
    return lines


def far_kernel(load_ref, far_ref):
    for y in range(4):
        for half in range(2):
            far_ref[2 * y + half] = load_ref[y, 4 + half]


def x_kernel(pops_ref, zp_ref, zm_ref, first_ref, second_ref, load_ref, up_ref, down_ref):
    columns = {1: (ZP, zp_ref[...]), -1: (ZM, zm_ref[...])}
    lines = y_lines(first_ref, second_ref)
    for y in range(4):
        for half in range(2):
            k = 2 * y + half
            up_ref[k] = load_ref[y, 2 + half]
            down_ref[k] = load_ref[y, 6 + half]
    for faces, out, x in ((XP, up_ref, 7), (XM, down_ref, 0)):
        for q, i in enumerate(faces):
            out[8 + q] = along_y(along_z(pops_ref[i, x], i, x, columns), i, x, lines)


def arrived(came, kinds, k):
    zhi = lax.rem(lax.axis_index("gx"), 4)
    tile = None
    for (kind, ways), ref in zip(LONG, came):
        if kind in kinds:
            ends = [(g + by) % 4 for g, by in ways.items()]
            ends = [end for end in ends if end not in PASSING.get(kind, ())]
            if not ends:
                continue
            if tile is None:
                tile = ref[k]
            else:
                tile = jnp.where(reduce(jnp.logical_or, [zhi == end for end in ends]), ref[k], tile)
    return tile


def collide_kernel(pops_ref, zp_ref, zm_ref, first_ref, second_ref, *refs):
    *came, out_ref = refs
    columns = {1: (ZP, zp_ref[...]), -1: (ZM, zm_ref[...])}
    lines = y_lines(first_ref, second_ref)
    for x in range(8):
        read = []
        for i, (cx, cy, cz) in enumerate(lattice_moves):
            source = x - cx
            if source < 0:
                tile = arrived(came, ("up",), 8 + XP.index(i))
            elif source > 7:
                tile = arrived(came, ("down",), 8 + XM.index(i))
            else:
                tile = along_y(along_z(pops_ref[i, source], i, source, columns), i, source, lines)
            read.append(tile)
        density, ux, uy, uz = momenta(read)
        common = 1.0 - 1.5 * (ux * ux + uy * uy + uz * uz)
        scaled = {w: (relaxation * w) * density for w in sorted(set(lattice_weights))}
        keep = 1.0 - relaxation
        out_ref[0, x] = keep * read[0] + scaled[lattice_weights[0]] * common
        for i in range(1, 19, 2):
            projected = None
            for c, u in zip(lattice_moves[i], (ux, uy, uz)):
                if c:
                    term = u if c == 1 else -u
                    projected = term if projected is None else projected + term
            weight = scaled[lattice_weights[i]]
            even = weight * (common + 4.5 * projected * projected)
            odd = weight * (3.0 * projected)
            out_ref[i, x] = keep * read[i] + (even + odd)
            out_ref[i + 1, x] = keep * read[i + 1] + (even - odd)


def post_kernel(load_ref, *refs):
    *came, out_ref, parcels = refs
    zhi = lax.rem(lax.axis_index("gx"), 4)
    for shift, kinds in zip(SHIFTS, ((), ("up",), ("far", "relay"), ("down",))):
        slot = lax.rem(zhi + (4 - shift), 4)
        for k in range(8):
            parcels[slot, k] = arrived(came, kinds, k) if shift else load_ref[k // 2, k % 2]
    for half in range(2):
        tiles = [parcels[part % 4, part // 4 * 2 + half] for part in range(16)]
        for k, tile in enumerate(swap_lane_groups(tiles, 8)):
            out_ref[2 * half + k // 8, k % 8] = tile


def call(kernel, out_shapes, args, scratch=()):
    vmem = pl.BlockSpec(memory_space=pltpu.VMEM)
    return pl.pallas_call(
        kernel,
        out_shape=[jax.ShapeDtypeStruct(s, f32) for s in out_shapes],
        in_specs=[vmem] * len(args),
        out_specs=[vmem] * len(out_shapes),
        scratch_shapes=list(scratch),
        compiler_params=pltpu.CompilerParams(vmem_limit_bytes=16 * 1024 * 1024),
    )(*args)


def shifted(x, axis, by):
    count = lax.axis_size(axis)
    return lax.ppermute(x, axis, [(i, (i + by) % count) for i in range(count)])


def hop(x, ways):
    pairs = [(g, (g + ways[g % 4]) % 16) for g in range(16) if g % 4 in ways]
    return lax.ppermute(x, "gx", pairs)


def swap(x, lower):
    pairs = [(i % 8, (i + 1) % 8) for i in range(lower, lower + 8, 2)]
    return lax.ppermute(x, "gy", pairs + [(j, i) for i, j in pairs])


def steps(populations):
    zp, zm = call(z_kernel, [TILE, TILE], (populations,))
    zp, zm = shifted(zp, "gz", 1), shifted(zm, "gz", -1)
    (load,) = call(pre_kernel, [(4, 8, 8, 128)], (populations,), [pltpu.VMEM((16, 2, 8, 128), f32)])
    groups = [[y * 4 + z for y in range(4)] for z in range(4)]
    load = lax.all_to_all(
        load.reshape(4, 8192), "gx", 0, 0, tiled=True, axis_index_groups=groups
    ).reshape(4, 8, 8, 128)
    first, second = call(
        y_kernel, [(5, 8, 128)] * 2, (populations, zp, zm), [pltpu.VMEM((2, 5, 8, 128), f32)]
    )
    first, second = swap(first, 7), swap(second, 0)
    (far,) = call(far_kernel, [(8, 8, 128)], (load,))
    up, down = call(
        x_kernel, [(13, 8, 128)] * 2, (populations, zp, zm, first, second, load)
    )
    message = {"up": up, "far": far, "down": down}
    came = []
    for kind, ways in LONG:
        came.append(hop(message[kind], ways))
        if kind == "far" and (0 in ways or 1 in ways):
            message["relay"] = came[-1]
    (populations_next,) = call(
        collide_kernel, [(19, 8, 8, 128)], (populations, zp, zm, first, second, *came)
    )
    (moments_slab,) = call(
        post_kernel, [(4, 8, 8, 128)], (load, *came), [pltpu.VMEM((4, 8, 8, 128), f32)]
    )
    return (populations_next, moments_slab)


def solution(mesh):
    return jax.shard_map(
        steps,
        mesh=mesh,
        in_specs=(P(None, "gx", "gy", "gz"),),
        out_specs=(P(None, "gx", "gy", "gz"), P(None, ("gz", "gx"), "gy", None)),
        check_vma=False,
    )
```

```python
from functools import reduce

import jax
import jax.numpy as jnp
from jax import lax
from jax.experimental import pallas as pl
from jax.experimental.pallas import tpu as pltpu
from jax.sharding import PartitionSpec as P


lattice_moves = [
    (0, 0, 0),
    (1, 0, 0),
    (-1, 0, 0),
    (0, 1, 0),
    (0, -1, 0),
    (0, 0, 1),
    (0, 0, -1),
    (1, 1, 0),
    (-1, -1, 0),
    (1, -1, 0),
    (-1, 1, 0),
    (1, 0, 1),
    (-1, 0, -1),
    (1, 0, -1),
    (-1, 0, 1),
    (0, 1, 1),
    (0, -1, -1),
    (0, 1, -1),
    (0, -1, 1),
]
lattice_weights = [1.0 / 3.0] + [1.0 / 18.0] * 6 + [1.0 / 36.0] * 12
relaxation = 1.6
TILE = (8, 128)
SHIFTS = (0, 1, 2, -1)
LONG = (('far', {2: 2, 3: 2, 0: -1}, None), ('up', {0: 1, 1: 1, 2: 1, 3: 1}, None), ('down', {0: -1, 1: -1, 2: -1, 3: -1}, None), ('far', {1: 1}, None), ('relay', {3: -1}, 0), ('relay', {2: 1}, 3))
PASSING = {"far": (2, 3)}
FAR_DOWN = (0,)
f32 = jnp.float32


def moving(axis, sign):
    return [i for i, move in enumerate(lattice_moves) if move[axis] == sign]


XP, XM = moving(0, 1), moving(0, -1)
YP, YM = moving(1, 1), moving(1, -1)
ZP, ZM = moving(2, 1), moving(2, -1)


def lanes():
    return lax.broadcasted_iota(jnp.int32, TILE, 1)


def rows():
    return lax.broadcasted_iota(jnp.int32, TILE, 0)


def roll_lanes(tile, shift):
    shift %= 128
    return pltpu.roll(tile, shift, axis=1) if shift else tile


def roll_rows(tile, shift):
    shift %= 8
    return pltpu.roll(tile, shift, axis=0) if shift else tile


def momenta(pieces):
    density = pieces[0]
    for piece in pieces[1:]:
        density = density + piece
    sums = []
    for axis in range(3):
        ups, downs = [pieces[i] for i in moving(axis, 1)], [pieces[i] for i in moving(axis, -1)]
        total = ups[0] - downs[0]
        for up, down in zip(ups[1:], downs[1:]):
            total = total + (up - down)
        sums.append(total)
    inverse = 1.0 / density
    return [density] + [total * inverse for total in sums]


def swap_lane_groups(tiles, width):
    tiles, step, lane = list(tiles), 1, lanes()
    while step < len(tiles):
        low = (lane // (width * step)) % 2 == 0
        for a in range(len(tiles)):
            if not a & step:
                b = a + step
                one, two = tiles[a], tiles[b]
                tiles[a] = jnp.where(low, one, roll_lanes(two, width * step))
                tiles[b] = jnp.where(low, roll_lanes(one, -width * step), two)
        step *= 2
    return tiles


def face_columns(pops_ref, faces, edge):
    tile = jnp.zeros(TILE, f32)
    for q, i in enumerate(faces):
        for x in range(8):
            column = q * 8 + x
            tile = jnp.where(lanes() == column, roll_lanes(pops_ref[i, x], column - edge), tile)
    return tile


def z_kernel(pops_ref, zp_ref, zm_ref):
    zp_ref[...] = face_columns(pops_ref, ZP, 127)
    zm_ref[...] = face_columns(pops_ref, ZM, 0)


def pre_kernel(pops_ref, load_ref, parcels):
    fields = [momenta([pops_ref[i, x] for i in range(19)]) for x in range(8)]
    planes = [swap_lane_groups([fields[x][m] for x in range(8)], 1) for m in range(4)]
    for half in range(2):
        sixteen = swap_lane_groups(planes[2 * half] + planes[2 * half + 1], 8)
        for part in range(16):
            parcels[part, half] = sixteen[part]
    zhi = lax.rem(lax.axis_index("gx"), 4)
    for y in range(4):
        for r, shift in enumerate(SHIFTS):
            if shift == 2:
                shift = jnp.where(reduce(jnp.logical_or, [zhi == g for g in FAR_DOWN]), -2, 2)
            part = lax.rem(zhi + (4 * y + shift + 16), 16)
            for half in range(2):
                load_ref[y, r * 2 + half] = parcels[part, half]


def along_z(tile, i, x, columns):
    cz = lattice_moves[i][2]
    if not cz:
        return tile
    faces, column = columns[cz]
    at, edge = faces.index(i) * 8 + x, 127 if cz == 1 else 0
    return roll_lanes(jnp.where(lanes() == edge, roll_lanes(column, edge - at), tile), cz)


def along_y(tile, i, x, lines):
    cy = lattice_moves[i][1]
    if not cy:
        return tile
    faces, tiles = lines[cy]
    line = jnp.broadcast_to(tiles[faces.index(i)][x : x + 1, :], TILE)
    return roll_rows(jnp.where(rows() == (7 if cy == 1 else 0), line, tile), cy)


def y_kernel(pops_ref, zp_ref, zm_ref, first_ref, second_ref, work_ref):
    columns = {1: (ZP, zp_ref[...]), -1: (ZM, zm_ref[...])}
    for faces, out, y in ((YP, work_ref.at[1], 7), (YM, work_ref.at[0], 0)):
        for q, i in enumerate(faces):
            tile = jnp.zeros(TILE, f32)
            for x in range(8):
                line = along_z(pops_ref[i, x], i, x, columns)
                tile = jnp.where(rows() == x, roll_rows(line, x - y), tile)
            out[q] = tile
    odd = lax.rem(lax.axis_index("gy"), 2)
    first_ref[...] = work_ref[odd]
    second_ref[...] = work_ref[1 - odd]


def y_lines(first_ref, second_ref):
    odd = lax.rem(lax.axis_index("gy"), 2) == 1
    lines = {}
    for sign, faces in ((1, YP), (-1, YM)):
        one, two = (first_ref, second_ref) if sign == 1 else (second_ref, first_ref)
        lines[sign] = (faces, [jnp.where(odd, two[q], one[q]) for q in range(5)])
    return lines


def far_kernel(load_ref, far_ref):
    for y in range(4):
        for half in range(2):
            far_ref[2 * y + half] = load_ref[y, 4 + half]


def x_kernel(pops_ref, zp_ref, zm_ref, first_ref, second_ref, load_ref, up_ref, down_ref):
    columns = {1: (ZP, zp_ref[...]), -1: (ZM, zm_ref[...])}
    lines = y_lines(first_ref, second_ref)
    for y in range(4):
        for half in range(2):
            k = 2 * y + half
            up_ref[k] = load_ref[y, 2 + half]
            down_ref[k] = load_ref[y, 6 + half]
    for faces, out, x in ((XP, up_ref, 7), (XM, down_ref, 0)):
        for q, i in enumerate(faces):
            out[8 + q] = along_y(along_z(pops_ref[i, x], i, x, columns), i, x, lines)


def arrived(came, kinds, k):
    zhi = lax.rem(lax.axis_index("gx"), 4)
    tile = None
    for (kind, ways, _), ref in zip(LONG, came):
        if kind in kinds:
            ends = [(g + by) % 4 for g, by in ways.items()]
            ends = [end for end in ends if end not in PASSING.get(kind, ())]
            if not ends:
                continue
            if tile is None:
                tile = ref[k]
            else:
                tile = jnp.where(reduce(jnp.logical_or, [zhi == end for end in ends]), ref[k], tile)
    return tile


def collide_kernel(pops_ref, zp_ref, zm_ref, first_ref, second_ref, came, out_ref):
    columns = {1: (ZP, zp_ref[...]), -1: (ZM, zm_ref[...])}
    lines = y_lines(first_ref, second_ref)
    for x in range(8):
        read = []
        for i, (cx, cy, cz) in enumerate(lattice_moves):
            source = x - cx
            if source < 0:
                tile = arrived(came, ("up",), 8 + XP.index(i))
            elif source > 7:
                tile = arrived(came, ("down",), 8 + XM.index(i))
            else:
                tile = along_y(along_z(pops_ref[i, source], i, source, columns), i, source, lines)
            read.append(tile)
        density, ux, uy, uz = momenta(read)
        common = 1.0 - 1.5 * (ux * ux + uy * uy + uz * uz)
        scaled = {w: (relaxation * w) * density for w in sorted(set(lattice_weights))}
        keep = 1.0 - relaxation
        out_ref[0, x] = keep * read[0] + scaled[lattice_weights[0]] * common
        for i in range(1, 19, 2):
            projected = None
            for c, u in zip(lattice_moves[i], (ux, uy, uz)):
                if c:
                    term = u if c == 1 else -u
                    projected = term if projected is None else projected + term
            weight = scaled[lattice_weights[i]]
            even = weight * (common + 4.5 * projected * projected)
            odd = weight * (3.0 * projected)
            out_ref[i, x] = keep * read[i] + (even + odd)
            out_ref[i + 1, x] = keep * read[i + 1] + (even - odd)


def post_kernel(load_ref, came, out_ref, parcels):
    zhi = lax.rem(lax.axis_index("gx"), 4)
    for shift, kinds in zip(SHIFTS, ((), ("up",), ("far", "relay"), ("down",))):
        slot = lax.rem(zhi + (4 - shift), 4)
        for k in range(8):
            parcels[slot, k] = arrived(came, kinds, k) if shift else load_ref[k // 2, k % 2]
    for half in range(2):
        tiles = [parcels[part % 4, part // 4 * 2 + half] for part in range(16)]
        for k, tile in enumerate(swap_lane_groups(tiles, 8)):
            out_ref[2 * half + k // 8, k % 8] = tile


def last_kernel(pops_ref, zp_ref, zm_ref, first_ref, second_ref, load_ref, *refs):
    *came, next_ref, slab_ref, parcels = refs
    collide_kernel(pops_ref, zp_ref, zm_ref, first_ref, second_ref, came, next_ref)
    post_kernel(load_ref, came, slab_ref, parcels)


def call(kernel, out_shapes, args, scratch=()):
    vmem = pl.BlockSpec(memory_space=pltpu.VMEM)
    return pl.pallas_call(
        kernel,
        out_shape=[jax.ShapeDtypeStruct(s, f32) for s in out_shapes],
        in_specs=[vmem] * len(args),
        out_specs=[vmem] * len(out_shapes),
        scratch_shapes=list(scratch),
        compiler_params=pltpu.CompilerParams(vmem_limit_bytes=16 * 1024 * 1024),
    )(*args)


def shifted(x, axis, by):
    count = lax.axis_size(axis)
    return lax.ppermute(x, axis, [(i, (i + by) % count) for i in range(count)])


def hop(x, ways):
    pairs = [(g, (g + ways[g % 4]) % 16) for g in range(16) if g % 4 in ways]
    return lax.ppermute(x, "gx", pairs)


def swap(x, lower):
    pairs = [(i % 8, (i + 1) % 8) for i in range(lower, lower + 8, 2)]
    return lax.ppermute(x, "gy", pairs + [(j, i) for i, j in pairs])


def steps(populations):
    zp, zm = call(z_kernel, [TILE, TILE], (populations,))
    zp, zm = shifted(zp, "gz", 1), shifted(zm, "gz", -1)
    (load,) = call(pre_kernel, [(4, 8, 8, 128)], (populations,), [pltpu.VMEM((16, 2, 8, 128), f32)])
    groups = [[y * 4 + z for y in range(4)] for z in range(4)]
    load = lax.all_to_all(
        load.reshape(4, 8192), "gx", 0, 0, tiled=True, axis_index_groups=groups
    ).reshape(4, 8, 8, 128)
    first, second = call(
        y_kernel, [(5, 8, 128)] * 2, (populations, zp, zm), [pltpu.VMEM((2, 5, 8, 128), f32)]
    )
    first, second = swap(first, 7), swap(second, 0)
    (far,) = call(far_kernel, [(8, 8, 128)], (load,))
    up, down = call(
        x_kernel, [(13, 8, 128)] * 2, (populations, zp, zm, first, second, load)
    )
    message = {"up": up, "far": far, "down": down}
    came = []
    for kind, ways, first_step in LONG:
        sent = message[kind] if first_step is None else came[first_step]
        came.append(hop(sent, ways))
    return call(
        last_kernel,
        [(19, 8, 8, 128), (4, 8, 8, 128)],
        (populations, zp, zm, first, second, load, *came),
        [pltpu.VMEM((4, 8, 8, 128), f32)],
    )


def on_device(populations):
    return tuple(steps(populations))


def solution(mesh):
    return jax.shard_map(
        on_device,
        mesh=mesh,
        in_specs=(P(None, "gx", "gy", "gz"),),
        out_specs=(P(None, "gx", "gy", "gz"), P(None, ("gz", "gx"), "gy", None)),
        check_vma=False,
    )
```

```python
from functools import reduce

import jax
import jax.numpy as jnp
from jax import lax
from jax.experimental import pallas as pl
from jax.experimental.pallas import tpu as pltpu
from jax.sharding import PartitionSpec as P


lattice_moves = [
    (0, 0, 0),
    (1, 0, 0),
    (-1, 0, 0),
    (0, 1, 0),
    (0, -1, 0),
    (0, 0, 1),
    (0, 0, -1),
    (1, 1, 0),
    (-1, -1, 0),
    (1, -1, 0),
    (-1, 1, 0),
    (1, 0, 1),
    (-1, 0, -1),
    (1, 0, -1),
    (-1, 0, 1),
    (0, 1, 1),
    (0, -1, -1),
    (0, 1, -1),
    (0, -1, 1),
]
lattice_weights = [1.0 / 3.0] + [1.0 / 18.0] * 6 + [1.0 / 36.0] * 12
relaxation = 1.6
TILE = (8, 128)
SHIFTS = (0, 1, 2, -1)
LONG = (('far', {2: 2, 3: 2, 0: -1}, None), ('up', {0: 1, 1: 1, 2: 1, 3: 1}, None), ('down', {0: -1, 1: -1, 2: -1, 3: -1}, None), ('far', {1: 1}, None), ('relay', {3: -1}, 0), ('relay', {2: 1}, 3))
PASSING = {"far": (2, 3)}
FAR_DOWN = (0,)
f32 = jnp.float32


def moving(axis, sign):
    return [i for i, move in enumerate(lattice_moves) if move[axis] == sign]


XP, XM = moving(0, 1), moving(0, -1)
YP, YM = moving(1, 1), moving(1, -1)
ZP, ZM = moving(2, 1), moving(2, -1)


def lanes():
    return lax.broadcasted_iota(jnp.int32, TILE, 1)


def rows():
    return lax.broadcasted_iota(jnp.int32, TILE, 0)


def roll_lanes(tile, shift):
    shift %= 128
    return pltpu.roll(tile, shift, axis=1) if shift else tile


def roll_rows(tile, shift):
    shift %= 8
    return pltpu.roll(tile, shift, axis=0) if shift else tile


def momenta(pieces):
    density = pieces[0]
    for piece in pieces[1:]:
        density = density + piece
    sums = []
    for axis in range(3):
        ups, downs = [pieces[i] for i in moving(axis, 1)], [pieces[i] for i in moving(axis, -1)]
        total = ups[0] - downs[0]
        for up, down in zip(ups[1:], downs[1:]):
            total = total + (up - down)
        sums.append(total)
    inverse = 1.0 / density
    return [density] + [total * inverse for total in sums]


def swap_lane_groups(tiles, width):
    tiles, step, lane = list(tiles), 1, lanes()
    while step < len(tiles):
        low = (lane // (width * step)) % 2 == 0
        for a in range(len(tiles)):
            if not a & step:
                b = a + step
                one, two = tiles[a], tiles[b]
                tiles[a] = jnp.where(low, one, roll_lanes(two, width * step))
                tiles[b] = jnp.where(low, roll_lanes(one, -width * step), two)
        step *= 2
    return tiles


def face_columns(pops_ref, faces, edge):
    tile = jnp.zeros(TILE, f32)
    for q, i in enumerate(faces):
        for x in range(8):
            column = q * 8 + x
            tile = jnp.where(lanes() == column, roll_lanes(pops_ref[i, x], column - edge), tile)
    return tile


def z_kernel(pops_ref, zp_ref, zm_ref):
    zp_ref[...] = face_columns(pops_ref, ZP, 127)
    zm_ref[...] = face_columns(pops_ref, ZM, 0)


def pre_kernel(pops_ref, load_ref, parcels):
    fields = [momenta([pops_ref[i, x] for i in range(19)]) for x in range(8)]
    planes = [swap_lane_groups([fields[x][m] for x in range(8)], 1) for m in range(4)]
    for half in range(2):
        sixteen = swap_lane_groups(planes[2 * half] + planes[2 * half + 1], 8)
        for part in range(16):
            parcels[part, half] = sixteen[part]
    zhi = lax.rem(lax.axis_index("gx"), 4)
    for y in range(4):
        for r, shift in enumerate(SHIFTS):
            if shift == 2:
                shift = jnp.where(reduce(jnp.logical_or, [zhi == g for g in FAR_DOWN]), -2, 2)
            part = lax.rem(zhi + (4 * y + shift + 16), 16)
            for half in range(2):
                load_ref[y, r * 2 + half] = parcels[part, half]


def along_z(tile, i, x, columns):
    cz = lattice_moves[i][2]
    if not cz:
        return tile
    faces, column = columns[cz]
    at, edge = faces.index(i) * 8 + x, 127 if cz == 1 else 0
    return roll_lanes(jnp.where(lanes() == edge, roll_lanes(column, edge - at), tile), cz)


def along_y(tile, i, x, lines):
    cy = lattice_moves[i][1]
    if not cy:
        return tile
    faces, tiles = lines[cy]
    line = jnp.broadcast_to(tiles[faces.index(i)][x : x + 1, :], TILE)
    return roll_rows(jnp.where(rows() == (7 if cy == 1 else 0), line, tile), cy)


def y_kernel(pops_ref, zp_ref, zm_ref, first_ref, second_ref, work_ref):
    columns = {1: (ZP, zp_ref[...]), -1: (ZM, zm_ref[...])}
    for faces, out, y in ((YP, work_ref.at[1], 7), (YM, work_ref.at[0], 0)):
        for q, i in enumerate(faces):
            tile = jnp.zeros(TILE, f32)
            for x in range(8):
                line = along_z(pops_ref[i, x], i, x, columns)
                tile = jnp.where(rows() == x, roll_rows(line, x - y), tile)
            out[q] = tile
    odd = lax.rem(lax.axis_index("gy"), 2)
    first_ref[...] = work_ref[odd]
    second_ref[...] = work_ref[1 - odd]


def y_lines(first_ref, second_ref):
    odd = lax.rem(lax.axis_index("gy"), 2) == 1
    lines = {}
    for sign, faces in ((1, YP), (-1, YM)):
        one, two = (first_ref, second_ref) if sign == 1 else (second_ref, first_ref)
        lines[sign] = (faces, [jnp.where(odd, two[q], one[q]) for q in range(5)])
    return lines


def far_kernel(load_ref, far_ref):
    for y in range(4):
        for half in range(2):
            far_ref[2 * y + half] = load_ref[y, 4 + half]


def x_kernel(pops_ref, zp_ref, zm_ref, first_ref, second_ref, load_ref, up_ref, down_ref):
    columns = {1: (ZP, zp_ref[...]), -1: (ZM, zm_ref[...])}
    lines = y_lines(first_ref, second_ref)
    for y in range(4):
        for half in range(2):
            k = 2 * y + half
            up_ref[k] = load_ref[y, 2 + half]
            down_ref[k] = load_ref[y, 6 + half]
    for faces, out, x in ((XP, up_ref, 7), (XM, down_ref, 0)):
        for q, i in enumerate(faces):
            out[8 + q] = along_y(along_z(pops_ref[i, x], i, x, columns), i, x, lines)


def arrived(came, kinds, k):
    zhi = lax.rem(lax.axis_index("gx"), 4)
    tile = None
    for (kind, ways, _), ref in zip(LONG, came):
        if kind in kinds:
            ends = [(g + by) % 4 for g, by in ways.items()]
            ends = [end for end in ends if end not in PASSING.get(kind, ())]
            if not ends:
                continue
            if tile is None:
                tile = ref[k]
            else:
                tile = jnp.where(reduce(jnp.logical_or, [zhi == end for end in ends]), ref[k], tile)
    return tile


def collide(pops_ref, zp_ref, zm_ref, first_ref, second_ref, came, out_ref, places, start):
    columns = {1: (ZP, zp_ref[...]), -1: (ZM, zm_ref[...])}
    lines = y_lines(first_ref, second_ref)
    for x in places:
        read = []
        for i, (cx, cy, cz) in enumerate(lattice_moves):
            source = x - cx
            if source < 0:
                tile = arrived(came, ("up",), 8 + XP.index(i))
            elif source > 7:
                tile = arrived(came, ("down",), 8 + XM.index(i))
            else:
                tile = along_y(along_z(pops_ref[i, source], i, source, columns), i, source, lines)
            read.append(tile)
        density, ux, uy, uz = momenta(read)
        common = 1.0 - 1.5 * (ux * ux + uy * uy + uz * uz)
        scaled = {w: (relaxation * w) * density for w in sorted(set(lattice_weights))}
        keep = 1.0 - relaxation
        out_ref[0, x - start] = keep * read[0] + scaled[lattice_weights[0]] * common
        for i in range(1, 19, 2):
            projected = None
            for c, u in zip(lattice_moves[i], (ux, uy, uz)):
                if c:
                    term = u if c == 1 else -u
                    projected = term if projected is None else projected + term
            weight = scaled[lattice_weights[i]]
            even = weight * (common + 4.5 * projected * projected)
            odd = weight * (3.0 * projected)
            out_ref[i, x - start] = keep * read[i] + (even + odd)
            out_ref[i + 1, x - start] = keep * read[i + 1] + (even - odd)


def post_kernel(load_ref, came, out_ref, parcels):
    zhi = lax.rem(lax.axis_index("gx"), 4)
    for shift, kinds in zip(SHIFTS, ((), ("up",), ("far", "relay"), ("down",))):
        slot = lax.rem(zhi + (4 - shift), 4)
        for k in range(8):
            parcels[slot, k] = arrived(came, kinds, k) if shift else load_ref[k // 2, k % 2]
    for half in range(2):
        tiles = [parcels[part % 4, part // 4 * 2 + half] for part in range(16)]
        for k, tile in enumerate(swap_lane_groups(tiles, 8)):
            out_ref[2 * half + k // 8, k % 8] = tile


def inner_kernel(pops_ref, zp_ref, zm_ref, first_ref, second_ref, out_ref):
    collide(pops_ref, zp_ref, zm_ref, first_ref, second_ref, (), out_ref, range(1, 7), 1)


def last_kernel(pops_ref, zp_ref, zm_ref, first_ref, second_ref, load_ref, inner_ref, *refs):
    *came, next_ref, slab_ref, parcels = refs
    next_ref[:, 1:7] = inner_ref[...]
    collide(pops_ref, zp_ref, zm_ref, first_ref, second_ref, came, next_ref, (0, 7), 0)
    post_kernel(load_ref, came, slab_ref, parcels)


def call(kernel, out_shapes, args, scratch=()):
    vmem = pl.BlockSpec(memory_space=pltpu.VMEM)
    return pl.pallas_call(
        kernel,
        out_shape=[jax.ShapeDtypeStruct(s, f32) for s in out_shapes],
        in_specs=[vmem] * len(args),
        out_specs=[vmem] * len(out_shapes),
        scratch_shapes=list(scratch),
        compiler_params=pltpu.CompilerParams(vmem_limit_bytes=16 * 1024 * 1024),
    )(*args)


def shifted(x, axis, by):
    count = lax.axis_size(axis)
    return lax.ppermute(x, axis, [(i, (i + by) % count) for i in range(count)])


def hop(x, ways):
    pairs = [(g, (g + ways[g % 4]) % 16) for g in range(16) if g % 4 in ways]
    return lax.ppermute(x, "gx", pairs)


def swap(x, lower):
    pairs = [(i % 8, (i + 1) % 8) for i in range(lower, lower + 8, 2)]
    return lax.ppermute(x, "gy", pairs + [(j, i) for i, j in pairs])


def steps(populations):
    zp, zm = call(z_kernel, [TILE, TILE], (populations,))
    zp, zm = shifted(zp, "gz", 1), shifted(zm, "gz", -1)
    (load,) = call(pre_kernel, [(4, 8, 8, 128)], (populations,), [pltpu.VMEM((16, 2, 8, 128), f32)])
    groups = [[y * 4 + z for y in range(4)] for z in range(4)]
    load = lax.all_to_all(
        load.reshape(4, 8192), "gx", 0, 0, tiled=True, axis_index_groups=groups
    ).reshape(4, 8, 8, 128)
    first, second = call(
        y_kernel, [(5, 8, 128)] * 2, (populations, zp, zm), [pltpu.VMEM((2, 5, 8, 128), f32)]
    )
    first, second = swap(first, 7), swap(second, 0)
    (far,) = call(far_kernel, [(8, 8, 128)], (load,))
    up, down = call(
        x_kernel, [(13, 8, 128)] * 2, (populations, zp, zm, first, second, load)
    )
    message = {"up": up, "far": far, "down": down}
    came = []
    for kind, ways, first_step in LONG:
        sent = message[kind] if first_step is None else came[first_step]
        came.append(hop(sent, ways))
    (inner,) = call(inner_kernel, [(19, 6, 8, 128)], (populations, zp, zm, first, second))
    return call(
        last_kernel,
        [(19, 8, 8, 128), (4, 8, 8, 128)],
        (populations, zp, zm, first, second, load, inner, *came),
        [pltpu.VMEM((4, 8, 8, 128), f32)],
    )


def on_device(populations):
    return tuple(steps(populations))


def solution(mesh):
    return jax.shard_map(
        on_device,
        mesh=mesh,
        in_specs=(P(None, "gx", "gy", "gz"),),
        out_specs=(P(None, "gx", "gy", "gz"), P(None, ("gz", "gx"), "gy", None)),
        check_vma=False,
    )
```
